32 devices in a mesh: dom: 32 (over z, y, x, core).
Axes of the slice: x: 2, y: 2, z: 4, core: 2. Of those that a mesh axis runs over, the one named last changes fastest.
Arguments:
- positions: float32 [3, 131072], P(None, 'dom'), may hold values from -1.5 to 1.5
- velocity: float32 [3, 131072], P(None, 'dom'), may hold values from -6 to 6
- density_weight: float32 [131072], P('dom'), may hold values from 0.5 to 2
- embed_strength: float32 [131072], P('dom'), may hold values from 0.5 to 2
- occupied: int32 [131072], P('dom'), may hold values 0 or 1
- send_list: int32 [32, 8, 8], P('dom'), may hold values from 0 to 31, as said below
- send_count: int32 [32, 8], P('dom'), may hold values from 0 to 8, as said below
- pair_tiles: int32 [1024, 24], P('dom'), may hold values from 0 to 95, as said below
- pair_count: int32 [1024], P('dom'), may hold values from 1 to 24, as said below
- migrate_dest: int32 [1024], P('dom'), may hold values from 0 to 31, as said below
Outputs:
- force: float32 [3, 131072], P(None, 'dom')
- energy: float32 [131072], P('dom')
- moved: float32 [7, 262144], P(None, 'dom')
- moved_count: int32 [32], P('dom')
The draws below stay inside these ranges and needn't reach their ends.
Inputs may be any that keep to these rules, and one draw needn't show every extreme that they name: `send_list`: for one domain and one offset the entries are distinct local tile indices. send_count[s, k] counts the tiles domain s sends to domain s - o_k; it is 0 where that domain does not exist and 8 for some pairs. `pair_tiles`: entries index the frame of the tile's domain; a tile's entries are distinct and its first entry is its own local index. `pair_count`: the first tile of every domain uses all 24 slots. `migrate_dest`: A tile's new domain is within 4 of its domain; at most 4 tiles go from one domain to any other, at most 64 tiles to one domain, and both bounds are reached in every draw.
All inputs are finite; a program needn't handle non-finite values. No bound on the sum of `occupied` on one device may be relied on, other than what follows from the above.
Results may differ from the reference program's by a relative error of at most 0.0003.
Values sent between devices are 32-bit elements; how exact they have to be, the bound alone decides.
A program may use at most 64 MiB of HBM per device.

```python
import math
import jax
import jax.numpy as jnp
from jax import lax

TILE = 128
TILES_DEV = 32
PAIRS = 24
GMAX = 8
RADIUS = 4
MMAX = 4
SPAN = 8
CAP = 64
DOMAINS = 32
TILES = 1024
ATOMS = 131072


def offset_list_drawn():
    return [position - RADIUS for position in range(RADIUS)] + [position + 1 for position in range(RADIUS)]


def draw_send_list(key, part):
    keys = jax.random.split(key, DOMAINS * SPAN)
    chosen = jax.vmap(lambda single: jax.random.permutation(single, TILES_DEV)[:GMAX])(keys)
    return chosen.reshape(DOMAINS, SPAN, GMAX).astype(jnp.int32)


def draw_send_count(key, part):
    offsets = jnp.array(offset_list_drawn(), dtype=jnp.int32)
    counts = jax.random.randint(jax.random.fold_in(key, 11), (DOMAINS, SPAN), 0, GMAX + 1).astype(jnp.int32)
    source = jnp.arange(DOMAINS, dtype=jnp.int32)[:, None]
    offset_ids = jnp.arange(SPAN, dtype=jnp.int32)[None, :]
    target = source - offsets[None, :]
    counts = jnp.where((source + offset_ids) % SPAN == 0, GMAX, counts)
    counts = jnp.where((target >= 0) & (target < DOMAINS), counts, 0)
    return counts.astype(jnp.int32)


def draw_pair_tiles(key, part):
    frame_size = TILES_DEV + SPAN * GMAX
    scores = jax.random.randint(jax.random.fold_in(key, 21), (TILES, frame_size), 0, 1 << 20).astype(jnp.int32)
    column = jnp.arange(frame_size, dtype=jnp.int32)[None, :]
    scores = scores * frame_size + column
    own_local = (jnp.arange(TILES, dtype=jnp.int32) % TILES_DEV)[:, None]
    scores = jnp.where(column == own_local, (1 << 20) * frame_size + frame_size, scores)
    chosen = jax.lax.top_k(scores, PAIRS)[1]
    return chosen.astype(jnp.int32)


def draw_pair_count(key, part):
    counts = jax.random.randint(jax.random.fold_in(key, 31), (TILES,), 1, PAIRS + 1).astype(jnp.int32)
    first = jnp.arange(TILES, dtype=jnp.int32) % TILES_DEV == 0
    return jnp.where(first, PAIRS, counts).astype(jnp.int32)


def draw_migrate_dest(key, part):
    offsets = jnp.array(offset_list_drawn(), dtype=jnp.int32)
    hottest = jax.random.randint(jax.random.fold_in(key, 41), (), RADIUS, DOMAINS - RADIUS).astype(jnp.int32)
    counts = jax.random.randint(jax.random.fold_in(key, 42), (DOMAINS, SPAN), 0, MMAX + 1).astype(jnp.int32)
    source = jnp.arange(DOMAINS, dtype=jnp.int32)[:, None]
    target = source + offsets[None, :]
    counts = jnp.where((target >= 0) & (target < DOMAINS), counts, 0)
    counts = jnp.where(target == hottest, MMAX, counts)
    counts = jnp.where(source == hottest, 0, counts)
    keys = jax.random.split(jax.random.fold_in(key, 43), DOMAINS)
    orders = jax.vmap(lambda single: jax.random.permutation(single, TILES_DEV))(keys).astype(jnp.int32)
    rank_of = jnp.argsort(orders, axis=1, stable=True).astype(jnp.int32)
    limits = jnp.cumsum(counts, axis=1).astype(jnp.int32)
    which = jnp.sum((rank_of[:, :, None] >= limits[:, None, :]).astype(jnp.int32), axis=2)
    strides = jnp.concatenate([offsets, jnp.zeros((1,), jnp.int32)])
    return (source + strides[which]).reshape(TILES).astype(jnp.int32)


def with_ends(values, stream_key, low, largest):
    index_at = [jax.random.randint(jax.random.fold_in(stream_key, axis), (), 0, length) for axis, length in enumerate(values.shape)]
    longest = values.shape.index(max(values.shape))
    beside = index_at[:longest] + [(index_at[longest] + 1) % values.shape[longest]] + index_at[longest + 1:]
    return values.at[tuple(index_at)].set(low).at[tuple(beside)].set(largest)


def shard_levels(key, shape, shards, smallest, high):
    def one(dim, blocks):
        steps = jax.random.uniform(jax.random.fold_in(jax.random.fold_in(key, 6), dim), (blocks,), jnp.float32, smallest / len(shards), high / len(shards))
        return jnp.repeat(jnp.exp(steps), shape[dim] // blocks).reshape((-1,) + (1,) * (len(shape) - dim - 1))

    factor_of = one(*shards[0])
    for cut in shards[1:]:
        factor_of = factor_of * one(*cut)
    return factor_of


def normal_values(rng, shape, spread, most, cuts=(), kind=jnp.bfloat16):
    loudness = shard_levels(rng, shape, cuts, -0.22, 0.18) if cuts else 1.0
    values = jax.random.normal(rng, shape, jnp.float32) * spread * loudness
    return jnp.minimum(jnp.maximum(values, -most), most).astype(kind)


def setup_inputs(seed: int = 0) -> dict:
    key_list = jax.random.split(jax.random.key(seed), 11)
    return {
        "positions": jnp.clip(jax.random.uniform(key_list[0], (3, ATOMS), jnp.float32, -1.5, 1.5) * shard_levels(key_list[0], (3, ATOMS), ((1, 32),), -0.4, 0.0), -1.5, 1.5),
        "velocity": normal_values(key_list[1], (3, ATOMS), 1.0, 6.0, ((1, 32),), jnp.float32),
        "density_weight": jnp.clip(jnp.exp(math.log(2.0) - 1.3862944 * jax.random.uniform(key_list[2], (ATOMS,), jnp.float32) ** shard_levels(key_list[2], (ATOMS,), ((0, 32),), -0.2, 0.2)), 0.5, 2.0),
        "embed_strength": jnp.clip(jnp.exp(math.log(2.0) - 1.3862944 * jax.random.uniform(key_list[3], (ATOMS,), jnp.float32) ** shard_levels(key_list[3], (ATOMS,), ((0, 32),), -0.2, 0.2)), 0.5, 2.0),
        "occupied": with_ends((jax.random.randint(key_list[4], (ATOMS,), 0, 4) < 3).astype(jnp.int32), jax.random.fold_in(key_list[4], 1), 0, 1),
        "send_list": draw_send_list(jax.random.fold_in(key_list[10], 71), 0),
        "send_count": draw_send_count(jax.random.fold_in(key_list[10], 71), 0),
        "pair_tiles": draw_pair_tiles(jax.random.fold_in(key_list[10], 71), 0),
        "pair_count": draw_pair_count(jax.random.fold_in(key_list[10], 71), 0),
        "migrate_dest": draw_migrate_dest(jax.random.fold_in(key_list[10], 71), 0),
    }


CUTOFF_SQUARE = 4.0
REPULSE = 0.05
TIME_STEP = 0.05
EXACT_PRODUCT = lax.Precision.HIGHEST

def offset_list():
    return [position - RADIUS for position in range(RADIUS)] + [position + 1 for position in range(RADIUS)]

def pair_weights(own_occ, near_occ, slot_list, used_count, tile_ids):
    tile_width = own_occ.shape[-1]
    used_mask = (jnp.arange(slot_list.shape[1], dtype=jnp.int32)[None, :] < used_count[:, None]).astype(jnp.float32)
    itself = (slot_list == tile_ids[:, None]).astype(jnp.float32)
    identity_mask = jnp.eye(tile_width, dtype=jnp.float32)
    weight = used_mask[:, :, None, None] * own_occ[:, None, :, None] * near_occ[:, :, None, :]
    return weight * (1.0 - itself[:, :, None, None] * identity_mask[None, None])

def closeness(own_pos, near_pos):
    distance = jnp.zeros(near_pos.shape[:2] + (own_pos.shape[2], near_pos.shape[3]), jnp.float32)
    for coordinate in range(3):
        difference = own_pos[:, None, coordinate, :, None] - near_pos[:, :, coordinate, None, :]
        distance = distance + difference * difference
    return jnp.maximum(1.0 - distance / CUTOFF_SQUARE, 0.0)

def density_terms(own_pos, own_occ, near_pos, near_chi, near_occ, slot_list, used_count, tile_ids):
    weight = pair_weights(own_occ, near_occ, slot_list, used_count, tile_ids)
    within = closeness(own_pos, near_pos)
    reach_cube = weight * within * within * within
    density = lax.optimization_barrier(jnp.sum(reach_cube * near_chi[:, :, None, :], axis=(1, 3)))
    pair_energy = lax.optimization_barrier(jnp.sum(reach_cube * within, axis=(1, 3)))
    return (density, pair_energy)

def force_terms(own_pos, own_occ, own_chi, own_slope, near_pos, near_chi, near_occ, near_slope, slot_list, used_count, tile_ids):
    weight = pair_weights(own_occ, near_occ, slot_list, used_count, tile_ids)
    within = closeness(own_pos, near_pos)
    square = within * within
    mixed_slope = own_slope[:, None, :, None] * near_chi[:, :, None, :] + near_slope[:, :, None, :] * own_chi[:, None, :, None]
    pair_coef = weight * (2.0 / CUTOFF_SQUARE) * (3.0 * square * mixed_slope + 4.0 * REPULSE * square * within)
    total_coef = lax.optimization_barrier(jnp.sum(pair_coef, axis=(1, 3)))
    pulled = jnp.einsum('bpij,bpcj->bci', pair_coef, near_pos, precision=EXACT_PRODUCT)
    return own_pos * total_coef[:, None, :] - pulled

def ghost_tiles(per_domain, send_list, send_count):
    domains = per_domain.shape[0]
    offsets = jnp.array(offset_list(), dtype=jnp.int32)
    source = jnp.arange(domains, dtype=jnp.int32)[:, None] + offsets[None, :]
    inside = (source >= 0) & (source < domains)
    clipped = jnp.clip(source, 0, domains - 1).astype(jnp.int32)
    offset_ids = jnp.arange(SPAN, dtype=jnp.int32)[None, :]
    tile_list = send_list[clipped, offset_ids]
    counts = send_count[clipped, offset_ids]
    live_mask = inside[:, :, None] & (jnp.arange(GMAX, dtype=jnp.int32)[None, None, :] < counts[:, :, None])
    picked = per_domain[clipped[:, :, None], tile_list]
    live_float = live_mask.astype(jnp.float32).reshape(live_mask.shape + (1,) * (picked.ndim - 3))
    return (picked * live_float).reshape((domains, SPAN * GMAX) + per_domain.shape[2:])

def reference(positions, velocity, density_weight, embed_strength, occupied, send_list, send_count, pair_tiles, pair_count, migrate_dest):
    domains = send_list.shape[0]
    tiles_here = pair_tiles.shape[0] // domains
    tile_width = TILE
    filled = occupied.astype(jnp.float32).reshape(domains, tiles_here, tile_width)
    pos_tiles = positions.reshape(3, domains, tiles_here, tile_width).transpose(1, 2, 0, 3)
    vel_tiles = velocity.reshape(3, domains, tiles_here, tile_width).transpose(1, 2, 0, 3)
    weight_tiles = density_weight.reshape(domains, tiles_here, tile_width)
    embed_tiles = embed_strength.reshape(domains, tiles_here, tile_width)
    packed = jnp.concatenate([pos_tiles, weight_tiles[:, :, None], filled[:, :, None]], axis=2)
    frame_tiles = jnp.concatenate([packed, ghost_tiles(packed, send_list, send_count)], axis=1)
    slot_tiles = pair_tiles.reshape(domains, tiles_here, PAIRS)
    used_tiles = pair_count.reshape(domains, tiles_here)
    tile_ids = jnp.arange(tiles_here, dtype=jnp.int32)

    def density_domain(batch_items):
        native, frames, slot_list, used_count = batch_items
        nearby = frames[slot_list]
        return density_terms(native[:, 0:3], native[:, 4], nearby[:, :, 0:3], nearby[:, :, 3], nearby[:, :, 4], slot_list, used_count, tile_ids)
    density, pair_energy = lax.map(density_domain, (packed, frame_tiles, slot_tiles, used_tiles))
    root_term = jnp.sqrt(1.0 + density)
    slope_tiles = -0.5 * embed_tiles * filled / root_term
    energy_tiles = filled * (-embed_tiles * root_term + 0.5 * REPULSE * pair_energy)
    slope_frame = jnp.concatenate([slope_tiles, ghost_tiles(slope_tiles, send_list, send_count)], axis=1)

    def force_domain(batch_items):
        native, frames, slot_list, used_count, own_slope, frame_slope = batch_items
        nearby = frames[slot_list]
        near_slope = frame_slope[slot_list]
        return force_terms(native[:, 0:3], native[:, 4], native[:, 3], own_slope, nearby[:, :, 0:3], nearby[:, :, 3], nearby[:, :, 4], near_slope, slot_list, used_count, tile_ids)
    force_tiles = lax.map(force_domain, (packed, frame_tiles, slot_tiles, used_tiles, slope_tiles, slope_frame))
    new_vel = vel_tiles + TIME_STEP * force_tiles
    new_pos = pos_tiles + TIME_STEP * new_vel
    payload = jnp.concatenate([new_pos, new_vel, filled[:, :, None]], axis=2).reshape(domains * tiles_here, 7, tile_width)
    onehot = (migrate_dest[:, None] == jnp.arange(domains, dtype=jnp.int32)[None, :]).astype(jnp.int32)
    before = (jnp.cumsum(onehot, axis=0) - onehot).astype(jnp.int32)
    slot_index = lax.optimization_barrier(jnp.sum(onehot * before, axis=1)).astype(jnp.int32)
    moved_tiles = jnp.zeros((domains * CAP, 7, tile_width), jnp.float32).at[migrate_dest * CAP + slot_index].set(payload)
    tile_atoms = lax.optimization_barrier(jnp.sum(occupied.reshape(domains * tiles_here, tile_width), axis=1)).astype(jnp.int32)
    moved_count = lax.optimization_barrier(jnp.sum(onehot * tile_atoms[:, None], axis=0)).astype(jnp.int32)
    force = force_tiles.transpose(2, 0, 1, 3).reshape(3, domains * tiles_here * tile_width)
    energy = energy_tiles.reshape(domains * tiles_here * tile_width)
    moved = moved_tiles.transpose(1, 0, 2).reshape(7, domains * CAP * tile_width)
    return (force, energy, moved, moved_count)
```

```python
import functools

import jax
import jax.numpy as jnp
from jax import lax
from jax.experimental import pallas as pl
from jax.experimental.pallas import tpu as pltpu
from jax.sharding import PartitionSpec as P

TILE = 128
RADIUS = 4
MMAX = 4
REPULSE = 0.05
TIME_STEP = 0.05
OUTSIDE = -1e9
BATCH = 16
PLANES = 4
NEAR_K = 64
PULL_K = 32
MESH = pl.DeviceIdType.MESH
OFFSETS = [position - RADIUS for position in range(RADIUS)] + [
    position + 1 for position in range(RADIUS)
]
VMEM = pl.BlockSpec(memory_space=pltpu.VMEM)
SMEM = pl.BlockSpec(memory_space=pltpu.SMEM)
WIDE = 60 * 1024 * 1024


def exists(device, domains):
    return jnp.logical_and(device >= 0, device < domains)


def greet(me, domains):
    barrier = pltpu.get_barrier_semaphore()
    for offset in OFFSETS:

        @pl.when(exists(me + offset, domains))
        def _():
            pl.semaphore_signal(
                barrier, inc=1, device_id=(me + offset,), device_id_type=MESH
            )


def greeted(me, domains):
    peers = jnp.minimum(me, RADIUS) + jnp.minimum(domains - 1 - me, RADIUS)
    pl.semaphore_wait(pltpu.get_barrier_semaphore(), peers)


def frame_kernel(
    domains,
    send_list,
    send_count,
    positions,
    density,
    occupied,
    dest,
    own,
    ghost,
    dests,
    outbox,
    dest_row,
    send_sem,
    recv_sem,
    dest_send,
    dest_recv,
):
    me = lax.axis_index("dom")
    greet(me, domains)
    tiles = own.shape[1]
    ghosts = send_list.shape[2]
    for t in range(tiles):
        for c in range(3):
            own[c, t : t + 1, :] = 0.5 * positions[c : c + 1, t * TILE : (t + 1) * TILE]
    own[3] = density[...] * occupied[...].astype(jnp.float32)
    dest_row[...] = jnp.full_like(dest_row, -1)
    dest_row[:, 0:tiles] = dest[...]
    for k in range(len(OFFSETS)):
        used = send_count[0, k]
        for g in range(ghosts):
            source = pl.ds(send_list[0, k, g], 1)
            for c in range(3):
                outbox[k, c, g : g + 1, :] = own[c, source, :]
            outbox[k, 3, g : g + 1, :] = jnp.where(g < used, own[3, source, :], 0.0)
    greeted(me, domains)
    for k, offset in enumerate(OFFSETS):

        @pl.when(exists(me - offset, domains))
        def _():
            pltpu.make_async_remote_copy(
                src_ref=outbox.at[k],
                dst_ref=ghost.at[k],
                send_sem=send_sem.at[k],
                recv_sem=recv_sem.at[k],
                device_id=(me - offset,),
                device_id_type=MESH,
            ).start()
            pltpu.make_async_remote_copy(
                src_ref=dest_row,
                dst_ref=dests.at[k],
                send_sem=dest_send.at[k],
                recv_sem=dest_recv.at[k],
                device_id=(me - offset,),
                device_id_type=MESH,
            ).start()

        @pl.when(jnp.logical_not(exists(me + offset, domains)))
        def _():
            ghost[k] = jnp.zeros(ghost.shape[1:], jnp.float32)
            dests[k] = jnp.full(dests.shape[1:], -1, jnp.int32)

    for k, offset in enumerate(OFFSETS):

        @pl.when(exists(me - offset, domains))
        def _():
            pltpu.make_async_copy(outbox.at[k], outbox.at[k], send_sem.at[k]).wait()
            pltpu.make_async_copy(dest_row, dest_row, dest_send.at[k]).wait()

        @pl.when(exists(me + offset, domains))
        def _():
            pltpu.make_async_copy(ghost.at[k], ghost.at[k], recv_sem.at[k]).wait()
            pltpu.make_async_copy(dests.at[k], dests.at[k], dest_recv.at[k]).wait()


def exchange_kernel(domains, sign, outbox, inbox, send_sem, recv_sem):
    me = lax.axis_index("dom")
    greet(me, domains)
    greeted(me, domains)
    for k, offset in enumerate(OFFSETS):

        @pl.when(exists(me + sign * offset, domains))
        def _():
            pltpu.make_async_remote_copy(
                src_ref=outbox.at[k],
                dst_ref=inbox.at[k],
                send_sem=send_sem.at[k],
                recv_sem=recv_sem.at[k],
                device_id=(me + sign * offset,),
                device_id_type=MESH,
            ).start()

    for k, offset in enumerate(OFFSETS):

        @pl.when(exists(me + sign * offset, domains))
        def _():
            pltpu.make_async_copy(outbox.at[k], outbox.at[k], send_sem.at[k]).wait()

        @pl.when(exists(me - sign * offset, domains))
        def _():
            pltpu.make_async_copy(inbox.at[k], inbox.at[k], recv_sem.at[k]).wait()


def exchange(blocks, domains, sign, collective_id):
    count = len(OFFSETS)
    return pl.pallas_call(
        functools.partial(exchange_kernel, domains, sign),
        out_shape=jax.ShapeDtypeStruct(blocks.shape, blocks.dtype),
        in_specs=[VMEM],
        out_specs=VMEM,
        scratch_shapes=[
            pltpu.SemaphoreType.DMA((count,)),
            pltpu.SemaphoreType.DMA((count,)),
        ],
        compiler_params=pltpu.CompilerParams(
            collective_id=collective_id, has_side_effects=True
        ),
        name=f"exchange_{collective_id}",
    )(blocks)


def split(x):
    high = x.astype(jnp.bfloat16).astype(jnp.float32)
    rest = x - high
    middle = rest.astype(jnp.bfloat16).astype(jnp.float32)
    return high, middle, rest - middle


def left(parts):
    a, b, c = parts
    return [a, a, b, b, a, c]


def right(parts):
    a, b, c = parts
    return [a, b, a, b, c, a]


def near_rows(x, y, z, weight):
    square = x * x + y * y + z * z
    norm = jnp.where(weight > 0, 1.0 - square, OUTSIDE)
    ones = jnp.ones_like(x)
    rows = []
    for value in (x, y, z):
        rows += left(split(value))
    rows += list(split(norm)) + [ones] * 3
    return rows, norm


def scaled_rows(x, y, z, weight, norm):
    rows = []
    for value in (x, y, z):
        rows += left(split(weight * value))
    return rows + list(split(weight * norm)) + left(split(weight))


def mine_rows(x, y, z):
    square = x * x + y * y + z * z
    ones = jnp.ones_like(x)
    rows = []
    for value in (x, y, z):
        rows += right(split(2.0 * value))
    minus = split(-square)
    return rows + [ones] * 3, minus


def put_rows(table, first, depth, offset, rows):
    for r, row in enumerate(rows):
        table[pl.ds(first * depth + offset + r, 8, stride=depth), :] = row


def walk(pair_tiles, pair_count, null, item):
    tiles, most = pair_count.shape[0], pair_tiles.shape[0]
    total = jnp.int32(0)
    for t in range(tiles):
        total = total + pair_count[t]

    def step(_, where):
        t, p = where
        for _ in range(BATCH):
            mine = jnp.minimum(t, tiles - 1)
            near = jnp.where(t < tiles, pair_tiles[p, mine], null)
            item(mine, near)
            last = p + 1 >= pair_count[mine]
            p = jnp.where(last, 0, p + 1)
            t = jnp.where(last, t + 1, t)
        return t, p

    lax.fori_loop(
        0, (total + BATCH - 1) // BATCH, step, (jnp.int32(0), jnp.int32(0))
    )


def folded(sums, n, g):
    total = None
    for s in range(8):
        part = sums[n, pl.ds(g * 64 + s, 8, stride=8), :]
        total = part if total is None else total + part
    return total


def fold(values):
    return jnp.sum(values.reshape(values.shape[0] // 8, 8, TILE), axis=0)


def frame_groups(own, ghost):
    tiles = own.shape[1]
    for g in range(tiles // 8):
        yield g * 8, [own[c, g * 8 : g * 8 + 8, :] for c in range(PLANES)]
    for k in range(ghost.shape[0]):
        yield tiles + k * 8, [ghost[k, c] for c in range(PLANES)]
    yield tiles + ghost.shape[0] * 8, [jnp.zeros((8, TILE), jnp.float32)] * PLANES


def turn(stage, depth, lefts):
    group = 4

    def step(b, carry):
        for f in range(group):
            tile = b * group + f
            block = stage[pl.ds(pl.multiple_of(tile * depth, depth), depth), :]
            lefts[tile] = block.T
        return carry

    lax.fori_loop(0, lefts.shape[0] // group, step, 0)


def density_kernel(
    pair_tiles,
    pair_count,
    send_list,
    own,
    ghost,
    embed,
    energy,
    slope,
    outbox,
    stage,
    lefts,
    rights,
    sums,
):
    tiles = own.shape[1]
    null = tiles + ghost.shape[0] * 8
    zero8 = jnp.zeros((8, TILE), jnp.float32)
    rights[...] = jnp.zeros_like(rights)
    sums[...] = jnp.zeros_like(sums)
    for first, (x, y, z, weight) in frame_groups(own, ghost):
        rows, norm = near_rows(x, y, z, weight)
        rows = rows + scaled_rows(x, y, z, weight, norm)
        rows = rows + [zero8] * (NEAR_K - len(rows))
        put_rows(stage, first, NEAR_K, 0, rows)
    for g in range(tiles // 8):
        rows, minus = mine_rows(*[own[c, g * 8 : g * 8 + 8, :] for c in range(3)])
        put_rows(rights.at[0], g * 8, NEAR_K, 0, rows + list(minus))
        put_rows(rights.at[1], g * 8, NEAR_K, 24, rows + right(minus))
    turn(stage, NEAR_K, lefts)

    def item(mine, near):
        block = pl.ds(pl.multiple_of(mine * NEAR_K, NEAR_K), NEAR_K)
        right_block = jnp.concatenate([rights[0, block, :], rights[1, block, :]], axis=1)
        both = jnp.dot(lefts[near], right_block, preferred_element_type=jnp.float32)
        reach = jnp.maximum(both[:, :TILE], 0.0)
        square = reach * reach
        rows = pl.ds(pl.multiple_of(mine * 8, 8), 8)
        sums[0, rows, :] += fold(square * both[:, TILE:])
        sums[1, rows, :] += fold(square * square)

    walk(pair_tiles, pair_count, null, item)
    for g in range(tiles // 8):
        rows = slice(g * 8, g * 8 + 8)
        weight = own[3, rows, :]
        filled = (weight > 0).astype(jnp.float32)
        rho = folded(sums, 0, g) - weight
        pair = folded(sums, 1, g) - filled
        root = jnp.sqrt(1.0 + rho)
        strength = embed[rows, :]
        slope[rows, :] = -0.5 * strength * filled / root
        energy[rows, :] = filled * (-strength * root + 0.5 * REPULSE * pair)
    for k in range(send_list.shape[1]):
        for g in range(send_list.shape[2]):
            outbox[k, g : g + 1, :] = slope[pl.ds(send_list[0, k, g], 1), :]


def force_kernel(
    domains,
    pair_tiles,
    pair_count,
    dest,
    own,
    ghost,
    slope,
    ghost_slope,
    positions,
    velocity,
    force,
    outbox,
    stay,
    stage,
    lefts,
    rights,
    sums,
    wide,
    tile_rows,
    ranks,
):
    me = lax.axis_index("dom")
    tiles = own.shape[1]
    spans = len(OFFSETS)
    null = tiles + ghost.shape[0] * 8
    zero8 = jnp.zeros((8, TILE), jnp.float32)
    rights[...] = jnp.zeros_like(rights)
    sums[...] = jnp.zeros_like(sums)
    for n, (first, (x, y, z, weight)) in enumerate(frame_groups(own, ghost)):
        if n < tiles // 8:
            tilt = slope[first : first + 8, :]
        elif n < tiles // 8 + spans:
            k = n - tiles // 8
            tilt = jnp.where(exists(me + OFFSETS[k], domains), ghost_slope[k], 0.0)
        else:
            tilt = zero8
        tilt = (0.75 / REPULSE) * tilt
        rows, _ = near_rows(x, y, z, weight)
        w1, w2, _ = split(weight)
        t1, t2, _ = split(tilt)
        rows = rows + [w1, w1, w2, t1, t1, t2] + [zero8] * 2
        put_rows(stage, first, PULL_K, 0, rows)
        if n < tiles // 8:
            rows, minus = mine_rows(x, y, z)
            rows = rows + list(minus)
            put_rows(rights.at[0], first, PULL_K, 0, rows)
            rows = rows + [t1, t2, t1, w1, w2, w1]
            put_rows(rights.at[1], first, PULL_K, 0, rows)
    turn(stage, PULL_K, lefts)
    row = lax.broadcasted_iota(jnp.int32, (PULL_K, 3 * TILE), 0)
    column = lax.broadcasted_iota(jnp.int32, (PULL_K, 3 * TILE), 1)
    pick = jnp.zeros((PULL_K, 3 * TILE), jnp.float32)
    for c in range(3):
        here = jnp.logical_and(column >= c * TILE, column < (c + 1) * TILE)
        for r in (0, 2, 5):
            pick = jnp.where(jnp.logical_and(here, row == 6 * c + r), 1.0, pick)

    def spread(b, carry):
        for f in range(4):
            tile = b * 4 + f
            out = jnp.dot(lefts[tile], pick, preferred_element_type=jnp.float32)
            for c in range(3):
                wide[tile, c] = out[:, c * TILE : (c + 1) * TILE]
        return carry

    lax.fori_loop(0, lefts.shape[0] // 4, spread, 0)
    for k in range(spans + 1):
        ranks[k] = 0

    def item(mine, near):
        block = pl.ds(pl.multiple_of(mine * PULL_K, PULL_K), PULL_K)
        right_block = jnp.concatenate([rights[0, block, :], rights[1, block, :]], axis=1)
        both = jnp.dot(lefts[near], right_block, preferred_element_type=jnp.float32)
        reach = jnp.maximum(both[:, :TILE], 0.0)
        coef = reach * reach * both[:, TILE:]
        rows = pl.ds(pl.multiple_of(mine * 8, 8), 8)
        for c in range(3):
            sums[c, rows, :] += fold(coef * wide[near, c])
        sums[3, rows, :] += fold(coef)

    walk(pair_tiles, pair_count, null, item)
    for t in range(tiles):
        for c in range(3):
            columns = slice(t * TILE, (t + 1) * TILE)
            tile_rows[c, t : t + 1, :] = positions[c : c + 1, columns]
            tile_rows[3 + c, t : t + 1, :] = velocity[c : c + 1, columns]
    packed = stage
    for g in range(tiles // 8):
        rows = slice(g * 8, g * 8 + 8)
        filled = (own[3, rows, :] > 0).astype(jnp.float32)
        total = folded(sums, 3, g)
        values = []
        for c in range(3):
            pull = (4.0 * REPULSE) * filled * (
                total * own[c, rows, :] - folded(sums, c, g)
            )
            tile_rows[6 + c, rows, :] = pull
            new_vel = tile_rows[3 + c, rows, :] + TIME_STEP * pull
            new_pos = tile_rows[c, rows, :] + TIME_STEP * new_vel
            put_rows(packed, g * 8, 8, c, [new_pos])
            put_rows(packed, g * 8, 8, 3 + c, [new_vel])
        put_rows(packed, g * 8, 8, 6, [filled, zero8])
    for t in range(tiles):
        for c in range(3):
            force[c : c + 1, t * TILE : (t + 1) * TILE] = tile_rows[6 + c, t : t + 1, :]

    def place_tile(t, carry):
        tile = packed[pl.ds(pl.multiple_of(t * 8, 8), 8), :]
        relative = dest[t] - me
        place = jnp.where(relative < 0, relative + RADIUS, relative + RADIUS - 1)
        place = jnp.where(relative == 0, spans, place)
        rank = ranks[place]
        ranks[place] = rank + 1

        @pl.when(relative == 0)
        def _():
            stay[rank] = tile

        @pl.when(relative != 0)
        def _():
            outbox[place, rank] = tile

        return carry

    lax.fori_loop(0, tiles, place_tile, 0)


def settle_kernel(dest, dests, inbox, stay, moved, count):
    me = lax.axis_index("dom")
    tiles, slots = dest.shape[0], moved.shape[1] // TILE
    rows = moved.shape[0]
    spans = len(OFFSETS)

    def put(e, tile, atoms):
        moved[:, pl.ds(pl.multiple_of(e * TILE, TILE), TILE)] = tile[0:rows]
        return atoms + tile

    def hits(value_of):
        total = jnp.int32(0)
        for i in range(tiles):
            total = total + (value_of(i) == me).astype(jnp.int32)
        return total

    slot = jnp.int32(0)
    atoms = jnp.zeros((8, TILE), jnp.float32)

    for k in range(spans):
        if k == RADIUS:
            here = hits(lambda i: dest[i])
            atoms = lax.fori_loop(
                0, here, lambda r, a, s=slot: put(s + r, stay[r], a), atoms
            )
            slot = slot + here
        here = hits(lambda i: dests[k, 0, i])
        atoms = lax.fori_loop(
            0, here, lambda r, a, s=slot: put(s + r, inbox[spans - 1 - k, r], a), atoms
        )
        slot = slot + here

    def clear(e, carry):
        moved[:, pl.ds(pl.multiple_of(e * TILE, TILE), TILE)] = jnp.zeros(
            (rows, TILE), jnp.float32
        )
        return carry

    lax.fori_loop(slot, slots, clear, 0)
    count[0] = jnp.sum(atoms[6:7]).astype(jnp.int32)


def per_device(
    positions,
    velocity,
    density_weight,
    embed_strength,
    occupied,
    send_list,
    send_count,
    pair_tiles,
    pair_count,
    migrate_dest,
):
    tiles = pair_tiles.shape[0]
    spans, ghosts = send_list.shape[1:]
    domains = lax.axis_size("dom")
    capacity = tiles + 2 * RADIUS * MMAX
    padded = tiles + spans * ghosts + 8
    f32, i32 = jnp.float32, jnp.int32

    def rows_of(flat):
        return flat.reshape(tiles, TILE)

    own, ghost, dests = pl.pallas_call(
        functools.partial(frame_kernel, domains),
        out_shape=(
            jax.ShapeDtypeStruct((PLANES, tiles, TILE), f32),
            jax.ShapeDtypeStruct((spans, PLANES, ghosts, TILE), f32),
            jax.ShapeDtypeStruct((spans, 1, TILE), i32),
        ),
        in_specs=[SMEM, SMEM, VMEM, VMEM, VMEM, VMEM],
        out_specs=(VMEM, VMEM, VMEM),
        scratch_shapes=[
            pltpu.VMEM((spans, PLANES, ghosts, TILE), f32),
            pltpu.VMEM((1, TILE), i32),
            pltpu.SemaphoreType.DMA((spans,)),
            pltpu.SemaphoreType.DMA((spans,)),
            pltpu.SemaphoreType.DMA((spans,)),
            pltpu.SemaphoreType.DMA((spans,)),
        ],
        compiler_params=pltpu.CompilerParams(collective_id=0, has_side_effects=True),
        name="frame",
    )(
        send_list,
        send_count,
        positions,
        rows_of(density_weight),
        rows_of(occupied),
        migrate_dest.reshape(1, tiles),
    )
    energy, slope, slope_out = pl.pallas_call(
        density_kernel,
        out_shape=(
            jax.ShapeDtypeStruct((tiles, TILE), f32),
            jax.ShapeDtypeStruct((tiles, TILE), f32),
            jax.ShapeDtypeStruct((spans, ghosts, TILE), f32),
        ),
        in_specs=[SMEM, SMEM, SMEM, VMEM, VMEM, VMEM],
        out_specs=(VMEM, VMEM, VMEM),
        scratch_shapes=[
            pltpu.VMEM((padded * NEAR_K, TILE), f32),
            pltpu.VMEM((padded, TILE, NEAR_K), f32),
            pltpu.VMEM((2, tiles * NEAR_K, TILE), f32),
            pltpu.VMEM((2, tiles * 8, TILE), f32),
        ],
        compiler_params=pltpu.CompilerParams(vmem_limit_bytes=WIDE),
        name="density",
    )(pair_tiles.T, pair_count, send_list, own, ghost, rows_of(embed_strength))
    ghost_slope = exchange(slope_out, domains, -1, 1)
    force, outbox, stay = pl.pallas_call(
        functools.partial(force_kernel, domains),
        out_shape=(
            jax.ShapeDtypeStruct(positions.shape, f32),
            jax.ShapeDtypeStruct((spans, MMAX, 8, TILE), f32),
            jax.ShapeDtypeStruct((tiles, 8, TILE), f32),
        ),
        in_specs=[SMEM, SMEM, SMEM] + [VMEM] * 6,
        out_specs=(VMEM, VMEM, VMEM),
        scratch_shapes=[
            pltpu.VMEM((padded * PULL_K, TILE), f32),
            pltpu.VMEM((padded, TILE, PULL_K), f32),
            pltpu.VMEM((2, tiles * PULL_K, TILE), f32),
            pltpu.VMEM((4, tiles * 8, TILE), f32),
            pltpu.VMEM((padded, 3, TILE, TILE), f32),
            pltpu.VMEM((9, tiles, TILE), f32),
            pltpu.SMEM((spans + 1,), i32),
        ],
        compiler_params=pltpu.CompilerParams(vmem_limit_bytes=WIDE),
        name="force",
    )(
        pair_tiles.T,
        pair_count,
        migrate_dest,
        own,
        ghost,
        slope,
        ghost_slope,
        positions,
        velocity,
    )
    inbox = exchange(outbox, domains, 1, 2)
    moved, moved_count = pl.pallas_call(
        settle_kernel,
        out_shape=(
            jax.ShapeDtypeStruct((7, capacity * TILE), f32),
            jax.ShapeDtypeStruct((1,), i32),
        ),
        in_specs=[SMEM, SMEM, VMEM, VMEM],
        out_specs=(VMEM, SMEM),
        name="settle",
    )(migrate_dest, dests, inbox, stay)
    return (force, energy.reshape(tiles * TILE), moved, moved_count)


def solution(mesh):
    placed = (
        P(None, "dom"),
        P(None, "dom"),
        P("dom"),
        P("dom"),
        P("dom"),
        P("dom", None, None),
        P("dom", None),
        P("dom", None),
        P("dom"),
        P("dom"),
    )
    return jax.shard_map(
        per_device,
        mesh=mesh,
        in_specs=placed,
        out_specs=(P(None, "dom"), P("dom"), P(None, "dom"), P("dom")),
        check_vma=False,
    )
```
